32 devices in a mesh: dom: 16 (over z, y, x), col: 2 (over core).
Axes of the slice: x: 2, y: 2, z: 4, core: 2. Of those that a mesh axis runs over, the one named last changes fastest.
Arguments:
- features: bfloat16 [16384, 256], P(('dom', 'col')), may hold values from -6 to 6
- weight: bfloat16 [256, 256], replicated, may hold values from -0.375 to 0.375
- cotangent: bfloat16 [16384, 256], P(('dom', 'col')), may hold values from -6 to 6
- tile_values: bfloat16 [1280, 128, 128], P(('dom', 'col')), may hold values from -0.15625 to 0.15625
- tile_rows: int32 [1280], P(('dom', 'col')), may hold values from 0 to 7
- tile_cols: int32 [1280], P(('dom', 'col')), may hold values from 0 to 19, as said below
- tile_count: int32 [32], P(('dom', 'col')), may hold values from 20 to 40, as said below
- send_blocks: int32 [32, 16], P(('dom', 'col')), may hold values from 0 to 3
Outputs:
- output_rows: bfloat16 [16384, 256], P(('dom', 'col'))
- feature_grad: bfloat16 [16384, 256], P(('dom', 'col'))
- weight_grad: float32 [256, 256], replicated
The draws below stay inside these ranges and needn't reach their ends.
Inputs may be any that keep to these rules, and one draw needn't show every extreme that they name: `tile_cols`: A value v below 4 names the device's own row block v; a value 4 + s names the row block that the device of partition s with the same col index sends to this partition; no receive slot is named by two tiles of one device. Only the first tile_count slots of a device's tiles are live; some device has all 40 live.
All inputs are finite; a program needn't handle non-finite values.
Results may differ from the reference program's by a relative error of at most 0.0049.
Values may be sent and summed in bfloat16 or wider, within the bound.
A program may use at most 128 MiB of HBM per device.

```python
import jax
import jax.numpy as jnp
from jax import lax

F_IN = 256
F_OUT = 256
BLK = 128
NB = 8
TILES = 40
NODES = 16384
N_DOM = 16
N_COL = 2


def draw_tile_cols(key, part):
    devices_all = N_DOM * N_COL
    half_blocks = NB // N_COL
    remote_count = min(N_DOM, 3 * TILES // 4)
    slot_keys = jax.random.split(jax.random.fold_in(key, 11), devices_all)
    slot_perms = jax.vmap(lambda k: jax.random.permutation(k, N_DOM))(slot_keys)
    remote = slot_perms[:, :remote_count] + half_blocks
    local_ids = jax.random.randint(jax.random.fold_in(key, 12), (devices_all, TILES - remote_count), 0, half_blocks)
    joined = jnp.concatenate([remote.astype(jnp.int32), local_ids.astype(jnp.int32)], axis=1)
    order_keys = jax.random.split(jax.random.fold_in(key, 13), devices_all)
    orders = jax.vmap(lambda k: jax.random.permutation(k, TILES))(order_keys)
    placed = jnp.take_along_axis(joined, orders.astype(jnp.int32), axis=1)
    return placed.reshape(devices_all * TILES).astype(jnp.int32)


def draw_tile_count(key, part):
    devices_all = N_DOM * N_COL
    base = jax.random.randint(jax.random.fold_in(key, 21), (devices_all,), 0, TILES)
    skewed = TILES // 2 + base * base // (2 * TILES)
    picked = jax.random.randint(jax.random.fold_in(key, 22), (), 0, devices_all)
    return jnp.where(jnp.arange(devices_all) == picked, TILES, skewed).astype(jnp.int32)


def set_ends(entries, own_key, least, high):
    longest = entries.shape.index(max(entries.shape))
    spots = []
    for shift in (0, 1):
        where = [jax.random.randint(jax.random.fold_in(own_key, axis), (), 0, length) for axis, length in enumerate(entries.shape)]
        where[longest] = (where[longest] + shift) % entries.shape[longest]
        spots.append(tuple(where))
    return entries.at[spots[0]].set(least).at[spots[1]].set(high)


def levels(stream_key, shape, cuts, low, top_value):
    gain = 1.0
    for axis_at, shards_of in cuts:
        heights = jax.random.uniform(jax.random.fold_in(jax.random.fold_in(stream_key, 6), axis_at), (shards_of,), jnp.float32, low / len(cuts), top_value / len(cuts))
        gain = gain * jnp.repeat(jnp.exp(heights), shape[axis_at] // shards_of).reshape((-1,) + (1,) * (len(shape) - 1 - axis_at))
    return gain


def bell_draw(key, shape, scale, reach, cuts=(), held_as=jnp.bfloat16):
    array = jax.random.normal(key, shape, jnp.float32) * scale
    if len(cuts) > 0:
        array = levels(key, shape, cuts, -0.22, 0.18) * array
    return jnp.clip(array, min=-reach, max=reach).astype(held_as)


def setup_inputs(seed: int = 0) -> dict:
    key_list = jax.random.split(jax.random.key(seed), 9)
    features = bell_draw(key_list[0], (NODES, F_IN), 1.0, 6.0, ((0, 32),))
    weight = bell_draw(key_list[1], (F_IN, F_OUT), F_IN ** -0.5, 0.375)
    cotangent = bell_draw(key_list[2], (NODES, F_OUT), 1.0, 6.0, ((0, 32),))
    tile_values = bell_draw(key_list[3], (N_DOM * N_COL * TILES, BLK, BLK), (10 * BLK) ** -0.5, 0.15625, ((0, 32),))
    tile_rows = set_ends(jax.random.randint(key_list[4], (N_DOM * N_COL * TILES,), 0, NB), jax.random.fold_in(key_list[4], 1), 0, NB - 1).astype(jnp.int32)
    tile_cols = draw_tile_cols(jax.random.fold_in(key_list[8], 71), 0)
    tile_count = draw_tile_count(jax.random.fold_in(key_list[8], 71), 0)
    send_blocks = set_ends(jax.random.randint(key_list[7], (N_DOM * N_COL, N_DOM), 0, NB // N_COL), jax.random.fold_in(key_list[7], 1), 0, (NB // N_COL) - 1).astype(jnp.int32)
    return dict(features=features, weight=weight, cotangent=cotangent, tile_values=tile_values, tile_rows=tile_rows, tile_cols=tile_cols, tile_count=tile_count, send_blocks=send_blocks)


def reference(features, weight, cotangent, tile_values, tile_rows, tile_cols, tile_count, send_blocks):
    devices_all = N_DOM * N_COL
    half_blocks = NB // N_COL
    total_blocks = NB * N_DOM
    blocks = features.reshape(total_blocks, BLK, F_IN)
    tiles = tile_values.reshape(devices_all, TILES, BLK, BLK)
    rows_local = tile_rows.reshape(devices_all, TILES).astype(jnp.int32)
    cols_local = tile_cols.reshape(devices_all, TILES).astype(jnp.int32)
    device_ids = jnp.arange(devices_all, dtype=jnp.int32)
    part_ids = (device_ids // N_COL)[:, None]
    core_ids = (device_ids % N_COL)[:, None]
    slots = jnp.clip(cols_local - half_blocks, 0, N_DOM - 1).astype(jnp.int32)
    sender = (slots * N_COL + core_ids).astype(jnp.int32)
    sent_ids = send_blocks.astype(jnp.int32)[sender, jnp.broadcast_to(part_ids, sender.shape)]
    remote_block = slots * NB + core_ids * half_blocks + sent_ids
    own_block = part_ids * NB + core_ids * half_blocks + cols_local
    global_cols = jnp.where(cols_local < half_blocks, own_block, remote_block).astype(jnp.int32)
    global_rows = (part_ids * NB + rows_local).astype(jnp.int32)
    live_mask = (jnp.arange(TILES, dtype=jnp.int32)[None, :] < tile_count.astype(jnp.int32)[:, None]).astype(jnp.float32)

    def forward_step(carry, inputs):
        tile_block, live_row, row_ids, col_ids = inputs
        weighted = tile_block.astype(jnp.float32) * live_row[:, None, None]
        picked = blocks[col_ids].astype(jnp.float32)
        terms = jnp.einsum("tij,tjf->tif", weighted, picked, precision=lax.Precision.HIGHEST)
        return carry.at[row_ids].add(terms), None

    hidden_sum, _ = lax.scan(forward_step, jnp.zeros((total_blocks, BLK, F_IN), jnp.float32),
                             (tiles, live_mask, global_rows, global_cols))
    hidden = hidden_sum.astype(jnp.bfloat16).reshape(NODES, F_IN)
    output_rows = jnp.dot(hidden, weight, preferred_element_type=jnp.float32).astype(jnp.bfloat16)
    grad_hidden = lax.dot_general(cotangent, weight, (((1,), (1,)), ((), ())),
                                  preferred_element_type=jnp.float32).astype(jnp.bfloat16)
    grad_blocks = grad_hidden.reshape(total_blocks, BLK, F_IN)

    def backward_step(carry, inputs):
        tile_block, live_row, row_ids, col_ids = inputs
        weighted = tile_block.astype(jnp.float32) * live_row[:, None, None]
        picked = grad_blocks[row_ids].astype(jnp.float32)
        terms = jnp.einsum("tji,tjf->tif", weighted, picked, precision=lax.Precision.HIGHEST)
        return carry.at[col_ids].add(terms), None

    grad_sum, _ = lax.scan(backward_step, jnp.zeros((total_blocks, BLK, F_IN), jnp.float32),
                           (tiles, live_mask, global_rows, global_cols))
    feature_grad = grad_sum.astype(jnp.bfloat16).reshape(NODES, F_IN)
    weight_grad = lax.dot_general(hidden, cotangent, (((0,), (0,)), ((), ())),
                                  preferred_element_type=jnp.float32)
    weight_grad = weight_grad * jnp.float32(1.0 / (NODES ** 0.5))
    return output_rows, feature_grad, weight_grad
```

```python
import functools

import jax
import jax.numpy as jnp
from jax import lax
from jax.experimental import pallas as pl
from jax.experimental.pallas import tpu as pltpu
from jax.sharding import PartitionSpec as P

MESH = pl.DeviceIdType.MESH
F32 = jnp.float32


def kernel(scale, rows_s, cols_s, count_s, send_s, feat, weight, cot, tiles_hbm,
           out, fgrad, wgrad,
           tiles, sendf, recvf, sendb, recvb, buf, base, gh, psend, precv, hid,
           wsend, wrecv, wchunk, wpart, wall, wpeer, tos,
           f_send, f_recv, b_send, b_recv, r_send, r_recv, g_send, g_recv, misc):
    slots = tiles.shape[0]
    half, blk, width = feat.shape
    n = recvf.shape[0]
    blocks = 2 * half
    me = lax.axis_index("dom")
    col = lax.axis_index("col")
    other = 1 - col
    count = count_s[0]

    def to_peer(k):
        return lax.rem(me + k, n)

    def from_peer(k):
        return lax.rem(me + n - k, n)

    def remote(src, dst, s_sem, r_sem, dom, core):
        return pltpu.make_async_remote_copy(
            src_ref=src, dst_ref=dst, send_sem=s_sem, recv_sem=r_sem,
            device_id=(dom, core), device_id_type=MESH)

    tile_copy = pltpu.make_async_copy(tiles_hbm, tiles, misc.at[0])
    tile_copy.start()

    barrier = pltpu.get_barrier_semaphore()

    def greet(k, carry):
        pl.semaphore_signal(barrier, inc=1, device_id=(to_peer(k), col), device_id_type=MESH)
        return carry

    lax.fori_loop(1, n, greet, 0)
    pl.semaphore_signal(barrier, inc=1, device_id=(me, other), device_id_type=MESH)

    def gather(k, carry):
        sendf[k] = feat[send_s[to_peer(k)]]
        return carry

    lax.fori_loop(1, n, gather, 0)
    recvf[me] = feat[send_s[me]]

    own = lax.dot_general(cot[...], weight[...], (((1,), (1,)), ((), ())),
                          preferred_element_type=F32).astype(jnp.bfloat16)
    gh[pl.ds(col * half, half)] = own.reshape(half, blk, width)

    def find(s, carry):
        found = jnp.int32(0)
        for t in range(slots):
            found = jnp.where((cols_s[t] == s + half) & (t < count), t + 1, found)
        tos[s] = found
        return carry

    lax.fori_loop(0, n, find, 0)

    pl.semaphore_wait(barrier, n)

    def f_copy(k, peer, slot):
        return remote(sendf.at[k], recvf.at[slot], f_send.at[k], f_recv.at[slot], peer, col)

    def b_copy(k, peer, slot):
        return remote(sendb.at[k], recvb.at[slot], b_send.at[k], b_recv.at[slot], peer, col)

    gh_half = gh.at[pl.ds(col * half, half)]
    gh_copy = remote(gh_half, gh_half, misc.at[1], misc.at[2], me, other)
    gh_copy.start()

    def f_start(k, carry):
        f_copy(k, to_peer(k), me).start()
        return carry

    lax.fori_loop(1, n, f_start, 0)

    buf[0] = jnp.zeros((blk, width), F32)
    tile_copy.wait()
    gh_copy.wait_send()
    gh_other = gh.at[pl.ds(other * half, half)]
    remote(gh_other, gh_other, misc.at[1], misc.at[2], me, other).wait_recv()

    def back_term(slot):
        found = tos[slot]
        at = jnp.maximum(found - 1, 0)
        term = lax.dot_general(tiles[at], gh[rows_s[at]], (((0,), (0,)), ((), ())),
                               preferred_element_type=F32)
        return jnp.where(found > 0, term, 0.0).astype(jnp.bfloat16)

    def b_start(k, carry):
        sendb[k] = back_term(to_peer(k))
        b_copy(k, to_peer(k), me).start()
        return carry

    lax.fori_loop(1, n, b_start, 0)
    recvb[me] = back_term(me)

    def link(lasts, key, index):
        prev = jnp.int32(0)
        for r, last in enumerate(lasts):
            prev = jnp.where(key == r, last, prev)
        return prev, tuple(jnp.where(key == r, index, last) for r, last in enumerate(lasts))

    def own_back(t, lasts):
        key = jnp.where(t < count, cols_s[t], -1)
        prev, lasts = link(lasts, key, t + 1)
        term = lax.dot_general(tiles[t], gh[rows_s[t]], (((0,), (0,)), ((), ())),
                               preferred_element_type=F32)
        buf[t + 1] = buf[prev] + term
        return lasts

    lasts = lax.fori_loop(0, slots, own_back, (jnp.int32(0),) * half)
    for j in range(half):
        base[j] = buf[lasts[j]]

    def own_fwd(t, lasts):
        source = cols_s[t]
        key = jnp.where((t < count) & (source < half), rows_s[t], -1)
        prev, lasts = link(lasts, key, t + 1)
        term = jnp.dot(tiles[t], feat[jnp.minimum(source, half - 1)], preferred_element_type=F32)
        buf[t + 1] = buf[prev] + term
        return lasts

    lasts = lax.fori_loop(0, slots, own_fwd, (jnp.int32(0),) * blocks)

    def slot_fwd(k, slot, lasts):
        found = tos[slot]
        at = jnp.maximum(found - 1, 0)
        key = jnp.where(found > 0, rows_s[at], -1)
        prev, lasts = link(lasts, key, slots + 1 + k)
        term = jnp.dot(tiles[at], recvf[slot], preferred_element_type=F32)
        buf[slots + 1 + k] = buf[prev] + term
        return lasts

    lasts = slot_fwd(0, me, lasts)

    def arrived(k, lasts):
        f_copy(k, from_peer(k), from_peer(k)).wait_recv()
        return slot_fwd(k, from_peer(k), lasts)

    lasts = lax.fori_loop(1, n, arrived, lasts)

    for j in range(half):
        psend[j] = buf[jnp.where(col == 0, lasts[half + j], lasts[j])]
    p_copy = remote(psend, precv, misc.at[3], misc.at[4], me, other)
    p_copy.start()
    p_copy.wait()
    for j in range(half):
        mine = buf[jnp.where(col == 0, lasts[j], lasts[half + j])]
        hid[pl.ds(j * blk, blk), :] = (mine + precv[j]).astype(jnp.bfloat16)

    local = lax.dot_general(hid[...], cot[...], (((0,), (0,)), ((), ())),
                            preferred_element_type=F32) * jnp.float32(scale)
    wh = width // 2
    low, high = local[:wh], local[wh:]
    wsend[...] = jnp.where(col == 0, high, low)
    w_copy = remote(wsend, wrecv, misc.at[5], misc.at[6], me, other)
    w_copy.start()
    out[...] = jnp.dot(hid[...], weight[...], preferred_element_type=F32).astype(jnp.bfloat16)
    w_copy.wait()
    share = jnp.where(col == 0, low, high) + wrecv[...]
    wchunk[...] = share.reshape(wchunk.shape)

    def r_copy(peer, chunk, slot):
        return remote(wchunk.at[chunk], wpart.at[slot], r_send.at[chunk], r_recv.at[slot], peer, col)

    def r_start(k, carry):
        r_copy(to_peer(k), to_peer(k), me).start()
        return carry

    lax.fori_loop(1, n, r_start, 0)
    wpart[me] = wchunk[me]

    def r_wait(k, carry):
        r_copy(from_peer(k), from_peer(k), from_peer(k)).wait_recv()
        return carry

    lax.fori_loop(1, n, r_wait, 0)
    wall[me] = jnp.sum(wpart[...], axis=0)

    def g_copy(k, peer, slot):
        return remote(wall.at[slot], wall.at[slot], g_send.at[k], g_recv.at[slot], peer, col)

    def g_start(k, carry):
        g_copy(k, to_peer(k), me).start()
        return carry

    lax.fori_loop(1, n, g_start, 0)

    def b_wait(k, carry):
        b_copy(k, from_peer(k), from_peer(k)).wait_recv()
        return carry

    lax.fori_loop(1, n, b_wait, 0)
    step = 16

    def total(i, carry):
        at = pl.ds(pl.multiple_of(i * step, step), step)

        def add(s, sums):
            value = recvb[s, at, :].astype(F32)
            home = send_s[s]
            return tuple(acc + jnp.where(home == j, value, 0.0) for j, acc in enumerate(sums))

        sums = lax.fori_loop(0, n, add, tuple(base[j, at, :] for j in range(half)), unroll=4)
        for j in range(half):
            fgrad[j, at, :] = sums[j].astype(jnp.bfloat16)
        return carry

    lax.fori_loop(0, blk // step, total, 0)

    def g_wait(k, carry):
        g_copy(k, from_peer(k), from_peer(k)).wait_recv()
        return carry

    lax.fori_loop(1, n, g_wait, 0)
    x_copy = remote(wall, wpeer, misc.at[7], misc.at[8], me, other)
    x_copy.start()

    def drain(k, carry):
        f_copy(k, to_peer(k), me).wait_send()
        b_copy(k, to_peer(k), me).wait_send()
        r_copy(to_peer(k), to_peer(k), me).wait_send()
        g_copy(k, to_peer(k), me).wait_send()
        return carry

    lax.fori_loop(1, n, drain, 0)
    wgrad[pl.ds(pl.multiple_of(col * wh, wh), wh), :] = wall[...].reshape(wh, wgrad.shape[1])
    x_copy.wait()
    wgrad[pl.ds(pl.multiple_of(other * wh, wh), wh), :] = wpeer[...].reshape(wh, wgrad.shape[1])


def local(features, weight, cotangent, tile_values, tile_rows, tile_cols, tile_count, send_blocks):
    slots, blk, _ = tile_values.shape
    rows, width = features.shape
    width_out = cotangent.shape[1]
    half = rows // blk
    n = send_blocks.shape[1]
    nodes = rows * lax.axis_size("col") * lax.axis_size("dom")
    scale = 1.0 / nodes**0.5
    bf = jnp.bfloat16
    chunk = width // 2 // n
    vmem = pl.BlockSpec(memory_space=pltpu.VMEM)
    smem = pl.BlockSpec(memory_space=pltpu.SMEM)
    sems = pltpu.SemaphoreType.DMA
    out, fgrad, wgrad = pl.pallas_call(
        functools.partial(kernel, scale),
        out_shape=(
            jax.ShapeDtypeStruct((rows, width_out), bf),
            jax.ShapeDtypeStruct((half, blk, width), bf),
            jax.ShapeDtypeStruct((width, width_out), F32),
        ),
        in_specs=[smem] * 4 + [vmem] * 3 + [pl.BlockSpec(memory_space=pl.ANY)],
        out_specs=(vmem, vmem, vmem),
        scratch_shapes=[
            pltpu.VMEM((slots, blk, blk), bf),
            pltpu.VMEM((n, blk, width), bf),
            pltpu.VMEM((n, blk, width), bf),
            pltpu.VMEM((n, blk, width), bf),
            pltpu.VMEM((n, blk, width), bf),
            pltpu.VMEM((slots + 1 + n, blk, width), F32),
            pltpu.VMEM((half, blk, width), F32),
            pltpu.VMEM((2 * half, blk, width), bf),
            pltpu.VMEM((half, blk, width), F32),
            pltpu.VMEM((half, blk, width), F32),
            pltpu.VMEM((rows, width), bf),
            pltpu.VMEM((width // 2, width_out), F32),
            pltpu.VMEM((width // 2, width_out), F32),
            pltpu.VMEM((n, chunk, width_out), F32),
            pltpu.VMEM((n, chunk, width_out), F32),
            pltpu.VMEM((n, chunk, width_out), F32),
            pltpu.VMEM((n, chunk, width_out), F32),
            pltpu.SMEM((n,), jnp.int32),
        ] + [sems((n,))] * 8 + [sems((9,))],
        compiler_params=pltpu.CompilerParams(
            collective_id=0, has_side_effects=True, vmem_limit_bytes=67000000),
    )(tile_rows, tile_cols, tile_count, send_blocks.reshape(n),
      features.reshape(half, blk, width), weight, cotangent, tile_values)
    return out, fgrad.reshape(rows, width), wgrad


def solution(mesh):
    return jax.shard_map(
        local,
        mesh=mesh,
        in_specs=(
            P(("dom", "col"), None),
            P(),
            P(("dom", "col"), None),
            P(("dom", "col"), None, None),
            P(("dom", "col")),
            P(("dom", "col")),
            P(("dom", "col")),
            P(("dom", "col"), None),
        ),
        out_specs=(P(("dom", "col"), None), P(("dom", "col"), None), P()),
        check_vma=False,
    )
```

```python
import functools

import jax
import jax.numpy as jnp
from jax import lax
from jax.experimental import pallas as pl
from jax.experimental.pallas import tpu as pltpu
from jax.sharding import PartitionSpec as P

MESH = pl.DeviceIdType.MESH
F32 = jnp.float32


def kernel(scale, rows_s, cols_s, count_s, send_s, feat_hbm, weight_hbm, cot_hbm, tiles_hbm,
           out, fgrad, wgrad,
           feat, weight, cot, tiles, sendf, recvf, sendb, recvb, buf, base, gh, psend, precv, hid,
           wsend, wrecv, wchunk, wpart, wall, wpeer, tos,
           f_send, f_recv, b_send, b_recv, r_send, r_recv, g_send, g_recv, misc):
    slots = tiles.shape[0]
    half, blk, width = feat.shape
    n = recvf.shape[0]
    blocks = 2 * half
    me = lax.axis_index("dom")
    col = lax.axis_index("col")
    other = 1 - col
    count = count_s[0]

    side = n // 2
    mine_side, spot = lax.div(me, side), lax.rem(me, side)

    def peer_side(k):
        return lax.rem(mine_side + 1 + lax.div(k - 1, side), 2) * side

    def to_peer(k):
        return peer_side(k) + lax.rem(spot + k, side)

    def from_peer(k):
        return peer_side(k) + lax.rem(spot + 2 * side - k, side)

    def remote(src, dst, s_sem, r_sem, dom, core):
        return pltpu.make_async_remote_copy(
            src_ref=src, dst_ref=dst, send_sem=s_sem, recv_sem=r_sem,
            device_id=(dom, core), device_id_type=MESH)

    feat_copy = pltpu.make_async_copy(feat_hbm, feat, misc.at[9])
    feat_copy.start()
    cot_copy = pltpu.make_async_copy(cot_hbm, cot, misc.at[10])
    cot_copy.start()
    weight_copy = pltpu.make_async_copy(weight_hbm, weight, misc.at[11])
    weight_copy.start()
    tile_copy = pltpu.make_async_copy(tiles_hbm, tiles, misc.at[0])
    tile_copy.start()

    barrier = pltpu.get_barrier_semaphore()

    def greet(k, carry):
        pl.semaphore_signal(barrier, inc=1, device_id=(to_peer(k), col), device_id_type=MESH)
        return carry

    lax.fori_loop(1, n, greet, 0)
    pl.semaphore_signal(barrier, inc=1, device_id=(me, other), device_id_type=MESH)

    feat_copy.wait()

    def gather(k, carry):
        sendf[k] = feat[send_s[to_peer(k)]]
        return carry

    lax.fori_loop(1, n, gather, 0)
    recvf[me] = feat[send_s[me]]

    cot_copy.wait()
    weight_copy.wait()
    own = lax.dot_general(cot[...], weight[...], (((1,), (1,)), ((), ())),
                          preferred_element_type=F32).astype(jnp.bfloat16)
    gh[pl.ds(col * half, half)] = own.reshape(half, blk, width)

    def find(s, carry):
        found = jnp.int32(0)
        for t in range(slots):
            found = jnp.where((cols_s[t] == s + half) & (t < count), t + 1, found)
        tos[s] = found
        return carry

    lax.fori_loop(0, n, find, 0)

    pl.semaphore_wait(barrier, n)

    def f_copy(k, peer, slot):
        return remote(sendf.at[k], recvf.at[slot], f_send.at[k], f_recv.at[slot], peer, col)

    def b_copy(k, peer, slot):
        return remote(sendb.at[k], recvb.at[slot], b_send.at[k], b_recv.at[slot], peer, col)

    gh_half = gh.at[pl.ds(col * half, half)]
    gh_copy = remote(gh_half, gh_half, misc.at[1], misc.at[2], me, other)
    gh_copy.start()

    def f_start(k, carry):
        f_copy(k, to_peer(k), me).start()
        return carry

    lax.fori_loop(1, n, f_start, 0)

    buf[0] = jnp.zeros((blk, width), F32)
    tile_copy.wait()
    gh_copy.wait_send()
    gh_other = gh.at[pl.ds(other * half, half)]
    remote(gh_other, gh_other, misc.at[1], misc.at[2], me, other).wait_recv()

    def back_term(slot):
        found = tos[slot]
        at = jnp.maximum(found - 1, 0)
        term = lax.dot_general(tiles[at], gh[rows_s[at]], (((0,), (0,)), ((), ())),
                               preferred_element_type=F32)
        return jnp.where(found > 0, term, 0.0).astype(jnp.bfloat16)

    def b_fill(k, carry):
        sendb[k] = back_term(to_peer(k))
        return carry

    lax.fori_loop(1, n, b_fill, 0)

    def b_start(k, carry):
        b_copy(k, to_peer(k), me).start()
        return carry

    cut1, cut2 = 1 + side // 2, 1 + 3 * side // 4
    ends = (1, cut1, cut2, side + 1)
    side_ends = (side + 1, side + side // 2, side + 3 * side // 4, n)

    def b_part(i):
        lax.fori_loop(ends[i], ends[i + 1], b_start, 0)
        lax.fori_loop(side_ends[i], side_ends[i + 1], b_start, 0)

    recvb[me] = back_term(me)

    def link(lasts, key, index):
        prev = jnp.int32(0)
        for r, last in enumerate(lasts):
            prev = jnp.where(key == r, last, prev)
        return prev, tuple(jnp.where(key == r, index, last) for r, last in enumerate(lasts))

    def own_back(t, lasts):
        key = jnp.where(t < count, cols_s[t], -1)
        prev, lasts = link(lasts, key, t + 1)
        term = lax.dot_general(tiles[t], gh[rows_s[t]], (((0,), (0,)), ((), ())),
                               preferred_element_type=F32)
        buf[t + 1] = buf[prev] + term
        return lasts

    lasts = lax.fori_loop(0, slots, own_back, (jnp.int32(0),) * half)
    for j in range(half):
        base[j] = buf[lasts[j]]

    def own_fwd(t, lasts):
        source = cols_s[t]
        key = jnp.where((t < count) & (source < half), rows_s[t], -1)
        prev, lasts = link(lasts, key, t + 1)
        term = jnp.dot(tiles[t], feat[jnp.minimum(source, half - 1)], preferred_element_type=F32)
        buf[t + 1] = buf[prev] + term
        return lasts

    lasts = lax.fori_loop(0, slots, own_fwd, (jnp.int32(0),) * blocks)

    b_part(0)

    def slot_fwd(k, slot, lasts):
        found = tos[slot]
        at = jnp.maximum(found - 1, 0)
        key = jnp.where(found > 0, rows_s[at], -1)
        prev, lasts = link(lasts, key, slots + 1 + k)
        term = jnp.dot(tiles[at], recvf[slot], preferred_element_type=F32)
        buf[slots + 1 + k] = buf[prev] + term
        return lasts

    lasts = slot_fwd(0, me, lasts)

    def arrived(i, lasts):
        k = n - i
        f_copy(k, from_peer(k), from_peer(k)).wait_recv()
        return slot_fwd(k, from_peer(k), lasts)

    lasts = lax.fori_loop(1, n, arrived, lasts)

    for j in range(half):
        psend[j] = buf[jnp.where(col == 0, lasts[half + j], lasts[j])]
    p_copy = remote(psend, precv, misc.at[3], misc.at[4], me, other)
    p_copy.start()
    p_copy.wait()
    for j in range(half):
        mine = buf[jnp.where(col == 0, lasts[j], lasts[half + j])]
        hid[pl.ds(j * blk, blk), :] = (mine + precv[j]).astype(jnp.bfloat16)

    local = lax.dot_general(hid[...], cot[...], (((0,), (0,)), ((), ())),
                            preferred_element_type=F32) * jnp.float32(scale)
    wh = width // 2
    low, high = local[:wh], local[wh:]
    wsend[...] = jnp.where(col == 0, high, low)
    w_copy = remote(wsend, wrecv, misc.at[5], misc.at[6], me, other)
    w_copy.start()
    out[...] = jnp.dot(hid[...], weight[...], preferred_element_type=F32).astype(jnp.bfloat16)
    w_copy.wait()
    share = jnp.where(col == 0, low, high) + wrecv[...]
    wchunk[...] = share.reshape(wchunk.shape)

    def r_copy(peer, chunk, slot):
        return remote(wchunk.at[chunk], wpart.at[slot], r_send.at[chunk], r_recv.at[slot], peer, col)

    def r_start(k, carry):
        r_copy(to_peer(k), to_peer(k), me).start()
        return carry

    lax.fori_loop(1, n, r_start, 0)
    b_part(1)
    wpart[me] = wchunk[me]

    def r_wait(k, carry):
        r_copy(from_peer(k), from_peer(k), from_peer(k)).wait_recv()
        return carry

    lax.fori_loop(1, n, r_wait, 0)
    wall[me] = jnp.sum(wpart[...], axis=0)

    def g_copy(k, peer, slot):
        return remote(wall.at[slot], wall.at[slot], g_send.at[k], g_recv.at[slot], peer, col)

    def g_start(k, carry):
        g_copy(k, to_peer(k), me).start()
        return carry

    lax.fori_loop(1, n, g_start, 0)
    b_part(2)

    def g_wait(k, carry):
        g_copy(k, from_peer(k), from_peer(k)).wait_recv()
        return carry

    lax.fori_loop(1, n, g_wait, 0)
    x_copy = remote(wall, wpeer, misc.at[7], misc.at[8], me, other)
    x_copy.start()
    wgrad[pl.ds(pl.multiple_of(col * wh, wh), wh), :] = wall[...].reshape(wh, wgrad.shape[1])

    def b_wait(k, carry):
        b_copy(k, from_peer(k), from_peer(k)).wait_recv()
        return carry

    lax.fori_loop(1, n, b_wait, 0)
    step = 16

    def total(i, carry):
        at = pl.ds(pl.multiple_of(i * step, step), step)

        def add(s, sums):
            value = recvb[s, at, :].astype(F32)
            home = send_s[s]
            return tuple(acc + jnp.where(home == j, value, 0.0) for j, acc in enumerate(sums))

        sums = lax.fori_loop(0, n, add, tuple(base[j, at, :] for j in range(half)), unroll=4)
        for j in range(half):
            fgrad[j, at, :] = sums[j].astype(jnp.bfloat16)
        return carry

    lax.fori_loop(0, blk // step, total, 0)

    def drain(k, carry):
        f_copy(k, to_peer(k), me).wait_send()
        b_copy(k, to_peer(k), me).wait_send()
        r_copy(to_peer(k), to_peer(k), me).wait_send()
        g_copy(k, to_peer(k), me).wait_send()
        return carry

    lax.fori_loop(1, n, drain, 0)
    x_copy.wait()
    wgrad[pl.ds(pl.multiple_of(other * wh, wh), wh), :] = wpeer[...].reshape(wh, wgrad.shape[1])


def place(*refs):
    count = (len(refs) - 1) // 3
    sources, targets, held, sem = refs[:count], refs[count:2 * count], refs[2 * count:-1], refs[-1]
    reads = [pltpu.make_async_copy(a, h, sem.at[i]) for i, (a, h) in enumerate(zip(sources, held))]
    writes = [pltpu.make_async_copy(h, b, sem.at[count + i]) for i, (h, b) in enumerate(zip(held, targets))]
    for read in reads:
        read.start()
    for read, write in zip(reads, writes):
        read.wait()
        write.start()
    for write in writes:
        write.wait()


def finish(*arrays):
    hbm = pl.BlockSpec(memory_space=pl.ANY)
    return pl.pallas_call(
        place,
        out_shape=tuple(jax.ShapeDtypeStruct(a.shape, a.dtype) for a in arrays),
        in_specs=[hbm] * len(arrays),
        out_specs=(hbm,) * len(arrays),
        scratch_shapes=[pltpu.VMEM(a.shape, a.dtype) for a in arrays]
        + [pltpu.SemaphoreType.DMA((2 * len(arrays),))],
    )(*arrays)


def local(features, weight, cotangent, tile_values, tile_rows, tile_cols, tile_count, send_blocks):
    slots, blk, _ = tile_values.shape
    rows, width = features.shape
    width_out = cotangent.shape[1]
    half = rows // blk
    n = send_blocks.shape[1]
    nodes = rows * lax.axis_size("col") * lax.axis_size("dom")
    scale = 1.0 / nodes**0.5
    bf = jnp.bfloat16
    chunk = width // 2 // n
    vmem = pl.BlockSpec(memory_space=pltpu.VMEM)
    hbm = pl.BlockSpec(memory_space=pl.ANY)
    smem = pl.BlockSpec(memory_space=pltpu.SMEM)
    sems = pltpu.SemaphoreType.DMA
    out, fgrad, wgrad = pl.pallas_call(
        functools.partial(kernel, scale),
        out_shape=(
            jax.ShapeDtypeStruct((rows, width_out), bf),
            jax.ShapeDtypeStruct((half, blk, width), bf),
            jax.ShapeDtypeStruct((width, width_out), F32),
        ),
        in_specs=[smem] * 4 + [hbm] * 4,
        out_specs=(vmem, vmem, vmem),
        scratch_shapes=[
            pltpu.VMEM((half, blk, width), bf),
            pltpu.VMEM((width, width_out), bf),
            pltpu.VMEM((rows, width_out), bf),
            pltpu.VMEM((slots, blk, blk), bf),
            pltpu.VMEM((n, blk, width), bf),
            pltpu.VMEM((n, blk, width), bf),
            pltpu.VMEM((n, blk, width), bf),
            pltpu.VMEM((n, blk, width), bf),
            pltpu.VMEM((slots + 1 + n, blk, width), F32),
            pltpu.VMEM((half, blk, width), F32),
            pltpu.VMEM((2 * half, blk, width), bf),
            pltpu.VMEM((half, blk, width), F32),
            pltpu.VMEM((half, blk, width), F32),
            pltpu.VMEM((rows, width), bf),
            pltpu.VMEM((width // 2, width_out), F32),
            pltpu.VMEM((width // 2, width_out), F32),
            pltpu.VMEM((n, chunk, width_out), F32),
            pltpu.VMEM((n, chunk, width_out), F32),
            pltpu.VMEM((n, chunk, width_out), F32),
            pltpu.VMEM((n, chunk, width_out), F32),
            pltpu.SMEM((n,), jnp.int32),
        ] + [sems((n,))] * 8 + [sems((12,))],
        compiler_params=pltpu.CompilerParams(
            collective_id=0, has_side_effects=True, vmem_limit_bytes=67000000),
    )(tile_rows, tile_cols, tile_count, send_blocks.reshape(n),
      features.reshape(half, blk, width), weight, cotangent, tile_values)
    return finish(out, fgrad.reshape(rows, width), wgrad)


def solution(mesh):
    return jax.shard_map(
        local,
        mesh=mesh,
        in_specs=(
            P(("dom", "col"), None),
            P(),
            P(("dom", "col"), None),
            P(("dom", "col"), None, None),
            P(("dom", "col")),
            P(("dom", "col")),
            P(("dom", "col")),
            P(("dom", "col"), None),
        ),
        out_specs=(P(("dom", "col"), None), P(("dom", "col"), None), P()),
        check_vma=False,
    )
```
